128 devices in a mesh: rep: 1, emb: 64 (over z, y, x), model: 2 (over core).
Axes of the slice: x: 4, y: 4, z: 4, core: 2. Of those that a mesh axis runs over, the one named last changes fastest.
Arguments:
- x: bfloat16 [128, 8192], P('rep')
- Wq: bfloat16 [8192, 8192], P('emb', 'model')
- Wk: bfloat16 [8192, 256], replicated
- Wv: bfloat16 [8192, 256], replicated
- Wo: bfloat16 [8192, 8192], P('model', 'emb')
- Kc: bfloat16 [128, 4096, 256], P('rep')
- Vc: bfloat16 [128, 4096, 256], P('rep')
- lengths: int32 [128], P('rep')
Outputs:
- output 1: bfloat16 [128, 8192], P('rep')
- output 2: bfloat16 [128, 256], P('rep')
- output 3: bfloat16 [128, 256], P('rep')
All inputs are finite; a program needn't handle non-finite values.
Results may differ from the reference program's by a relative error of at most 0.00955071.
Values are sent between devices in bfloat16 or wider.
A program may use at most 1.5 GiB of HBM per device.

```python
import jax
import jax.numpy as jnp
from jax import lax

B = 128
T = 4096
D = 8192
H = 32
DH = 256


def setup_inputs(seed: int = 0, part: int = 0) -> dict:
    kshared, kpart = jax.random.split(jax.random.key(seed))
    kpart = jax.random.fold_in(kpart, part)
    kq, kk, kv, ko = jax.random.split(kshared, 4)
    kx, kkc, kvc, kl = jax.random.split(kpart, 4)
    x = jax.random.normal(kx, (B, D), jnp.float32)
    Wq = jax.random.normal(kq, (D, H * DH), jnp.float32) * (2.5 * D ** -0.5)
    Wk = jax.random.normal(kk, (D, DH), jnp.float32) * D ** -0.5
    Wv = jax.random.normal(kv, (D, DH), jnp.float32) * D ** -0.5
    Wo = jax.random.normal(ko, (H * DH, D), jnp.float32) * (3.0 * (H * DH) ** -0.5)
    Kc = jax.random.normal(kkc, (B, T, DH), jnp.float32)
    Vc = jax.random.normal(kvc, (B, T, DH), jnp.float32)
    kl1, kl2, kl3 = jax.random.split(jax.random.fold_in(kl, 7), 3)
    full = T - 1 - jax.random.randint(kl1, (B,), 0, T // 8)
    tiny = jax.random.randint(kl2, (B,), 1, 9)
    lengths = jnp.where(jax.random.bernoulli(kl3, 0.5, (B,)), full, tiny).astype(jnp.int32)
    bf = jnp.bfloat16
    return {'x': x.astype(bf), 'Wq': Wq.astype(bf), 'Wk': Wk.astype(bf), 'Wv': Wv.astype(bf),
            'Wo': Wo.astype(bf), 'Kc': Kc.astype(bf), 'Vc': Vc.astype(bf), 'lengths': lengths}


def reference(x, Wq, Wk, Wv, Wo, Kc, Vc, lengths):
    scale = DH ** -0.5
    q = jnp.dot(x, Wq, preferred_element_type=jnp.float32).astype(jnp.bfloat16).reshape(B, H, DH)
    k_new = jnp.dot(x, Wk, preferred_element_type=jnp.float32).astype(jnp.bfloat16)
    v_new = jnp.dot(x, Wv, preferred_element_type=jnp.float32).astype(jnp.bfloat16)
    pos = jnp.arange(T)

    def one(a):
        qb, Kb, Vb, kn, vn, n = a
        s = jnp.dot(qb, Kb.T, preferred_element_type=jnp.float32) * scale
        s = jnp.where(pos[None, :] < n, s, -jnp.inf)
        sn = jnp.dot(qb, kn, preferred_element_type=jnp.float32) * scale
        m = jnp.maximum(jnp.max(s, axis=1), sn)
        p = jnp.exp(s - m[:, None])
        pn = jnp.exp(sn - m)
        l = jnp.sum(p, axis=1) + pn
        acc = jnp.dot(p.astype(jnp.bfloat16), Vb, preferred_element_type=jnp.float32)
        acc = acc + pn.astype(jnp.bfloat16).astype(jnp.float32)[:, None] * vn.astype(jnp.float32)[None, :]
        return (acc / l[:, None]).astype(jnp.bfloat16)

    o = lax.map(one, (q, Kc, Vc, k_new, v_new, lengths))
    y = x.astype(jnp.float32) + jnp.dot(o.reshape(B, H * DH), Wo, preferred_element_type=jnp.float32)
    return y.astype(jnp.bfloat16), k_new, v_new
```

```python
import functools

import jax
import jax.numpy as jnp
from jax import lax
from jax.experimental import pallas as pl
from jax.experimental.pallas import tpu as pltpu
from jax.sharding import PartitionSpec as P

F32 = jnp.float32
BF16 = jnp.bfloat16
L = 128


def _kernel(side, nm, x_h, wq_h, wk_h, wv_h, wo_h, kc_h, vc_h, len_s,
            y_h, kn_o, vn_o,
            x_v, xi_v, wq_v, wkv_v, wo_v, k_v, v_v,
            qp, rq, kva, s_v, o_v, og, t_v, yp, yx, yb, y_v,
            sem_l, sem_out, s_q, r_q, s_o, r_o, s_e, r_e, s_y, r_y, s_f, r_f):
    ne = side ** 3
    n = ne * nm
    B, D = x_v.shape
    DE = xi_v.shape[1]
    CQ = wq_v.shape[1]
    NT = CQ // L
    DH = k_v.shape[1]
    HL = CQ // DH
    T = k_v.shape[0]
    DC = wo_v.shape[1]
    bh = B // nm
    scale = DH ** -0.5

    e = lax.axis_index('emb')
    m = lax.axis_index('model')
    z, y, x = e // (side * side), (e // side) % side, e % side
    me = e * nm + m

    def peer(d):
        dm = d % nm
        c = d // nm
        pz = (z + c // (side * side)) % side
        py = (y + (c // side) % side) % side
        px = (x + c % side) % side
        pe = (pz * side + py) * side + px
        return pe, (m + dm) % nm, dm

    bar = pltpu.get_barrier_semaphore()

    @pl.loop(1, n)
    def _(d):
        pe, pm, _dm = peer(d)
        pl.semaphore_signal(bar, inc=1, device_id={'emb': pe, 'model': pm})

    col = pl.multiple_of(e * DE, DE)
    loads = [
        pltpu.make_async_copy(x_h.at[:, pl.ds(col, DE)], xi_v, sem_l.at[0]),
        pltpu.make_async_copy(wq_h, wq_v, sem_l.at[1]),
        pltpu.make_async_copy(x_h, x_v, sem_l.at[2]),
        pltpu.make_async_copy(wk_h, wkv_v.at[0], sem_l.at[3]),
        pltpu.make_async_copy(wv_h, wkv_v.at[1], sem_l.at[4]),
        pltpu.make_async_copy(kc_h.at[me], k_v, sem_l.at[5]),
        pltpu.make_async_copy(vc_h.at[me], v_v, sem_l.at[6]),
        pltpu.make_async_copy(wo_h, wo_v, sem_l.at[7]),
    ]
    for c in loads:
        c.start()
    loads[0].wait()
    loads[1].wait()

    GN = 4
    for j0 in range(0, NT, GN):
        t = jnp.dot(xi_v[...], wq_v[:, j0 * L:(j0 + GN) * L], preferred_element_type=F32)
        for u in range(GN):
            j = j0 + u
            per = DH // L
            row = (j % per) * HL + j // per
            qp[pl.ds(row, B, stride=NT), :] = t[:, u * L:(u + 1) * L]

    pl.semaphore_wait(bar, n - 1)

    @pl.loop(1, n)
    def _(d):
        pe, pm, _dm = peer(d)
        b = pe * nm + pm
        pltpu.make_async_remote_copy(
            src_ref=qp.at[pl.ds(pl.multiple_of(b * NT, NT), NT)],
            dst_ref=rq.at[pl.ds(pl.multiple_of(d * NT, NT), NT)],
            send_sem=s_q, recv_sem=r_q,
            device_id={'emb': pe, 'model': pm},
        ).start()

    loads[2].wait()
    loads[3].wait()
    loads[4].wait()
    KB = min(1024, D)
    kva[...] = jnp.zeros_like(kva)

    @pl.loop(0, D // KB)
    def _(kk):
        o = pl.multiple_of(kk * KB, KB)
        xs = x_v[:, pl.ds(o, KB)]
        kva[0] += jnp.dot(xs, wkv_v[0, pl.ds(o, KB), :], preferred_element_type=F32)
        kva[1] += jnp.dot(xs, wkv_v[1, pl.ds(o, KB), :], preferred_element_type=F32)

    kn_o[...] = kva[0].astype(BF16)
    vn_o[...] = kva[1].astype(BF16)
    loads[5].wait()
    loads[6].wait()

    rest = rq.at[pl.ds(NT, (n - 1) * NT)]
    pltpu.make_async_copy(rest, rest, r_q).wait()

    own = qp[pl.ds(pl.multiple_of(me * NT, NT), NT), :]

    def add(c, acc):
        a0, a1 = acc
        base = pl.multiple_of(c * nm * NT, NT)
        return (a0 + rq[pl.ds(base, NT), :], a1 + rq[pl.ds(base + NT, NT), :])

    a0, a1 = lax.fori_loop(1, ne, add, (own, rq[pl.ds(NT, NT), :]))
    per = DH // L
    q = jnp.concatenate(
        [jnp.concatenate([a[u * HL:(u + 1) * HL] for u in range(per)], axis=1) for a in (a0, a1)],
        axis=0).astype(BF16)

    kn = kva[0, pl.ds(me, 1), :].astype(BF16).astype(F32)
    vn = kva[1, pl.ds(me, 1), :].astype(BF16).astype(F32)
    sn = jnp.sum(q.astype(F32) * kn, axis=1, keepdims=True) * scale
    ln = len_s[me]
    TB = min(1024, T)
    mx = sn
    for t0 in range(0, T, TB):
        s = lax.dot_general(q, k_v[t0:t0 + TB, :], (((1,), (1,)), ((), ())),
                            preferred_element_type=F32) * scale
        pos = lax.broadcasted_iota(jnp.int32, s.shape, 1) + t0
        s = jnp.where(pos < ln, s, -jnp.inf)
        s_v[:, t0:t0 + TB] = s
        mx = jnp.maximum(mx, jnp.max(s, axis=1, keepdims=True))
    pn = jnp.exp(sn - mx)
    l = pn
    acc = pn.astype(BF16).astype(F32) * vn
    for t0 in range(0, T, TB):
        p = jnp.exp(s_v[:, t0:t0 + TB] - mx)
        l = l + jnp.sum(p, axis=1, keepdims=True)
        acc = acc + jnp.dot(p.astype(BF16), v_v[t0:t0 + TB, :], preferred_element_type=F32)
    o_v[...] = (acc / l).astype(BF16).reshape(nm, HL, DH)

    @pl.loop(1, n)
    def _(d):
        pe, pm, dm = peer(d)
        pltpu.make_async_remote_copy(
            src_ref=o_v.at[dm], dst_ref=og.at[me], send_sem=s_o, recv_sem=r_o,
            device_id={'emb': pe, 'model': pm},
        ).start()

    og[me] = o_v[0]
    loads[7].wait()
    most = og.at[pl.ds(0, n - 1)]
    pltpu.make_async_copy(most, most, r_o).wait()

    @pl.loop(0, B)
    def _(b):
        v = og[b].astype(F32)
        r = pl.multiple_of(b * HL, HL)
        for u in range(per):
            t_v[u, pl.ds(r, HL), :] = v[:, u * L:(u + 1) * L]

    ya = jnp.zeros((B, DC), F32)
    for h in range(HL):
        lhs = jnp.concatenate(
            [t_v[u, pl.ds(h, B, stride=HL), :] for u in range(per)], axis=1).astype(BF16)
        ya = ya + jnp.dot(lhs, wo_v[h * DH:(h + 1) * DH, :], preferred_element_type=F32)
    yp[...] = ya

    om = (m + 1) % nm
    ex = pltpu.make_async_remote_copy(
        src_ref=yp.at[pl.ds(pl.multiple_of(om * bh, bh), bh)], dst_ref=yx, send_sem=s_e, recv_sem=r_e,
        device_id={'emb': e, 'model': om})
    ex.start()
    ex.wait_recv()
    rows = pl.ds(pl.multiple_of(m * bh, bh), bh)
    yb[...] = (xi_v[rows, :].astype(F32) + (yp[rows, :] + yx[...])).astype(BF16)

    ycol = pl.ds(pl.multiple_of(e * DC, DC), DC)

    @pl.loop(1, ne)
    def _(c):
        pe, pm, _dm = peer(c * nm)
        pltpu.make_async_remote_copy(
            src_ref=yb, dst_ref=y_v.at[rows, ycol], send_sem=s_y, recv_sem=r_y,
            device_id={'emb': pe, 'model': pm},
        ).start()

    y_v[rows, ycol] = yb[...]
    got = y_v.at[pl.ds(0, bh), pl.ds(0, (ne - 1) * DC)]
    pltpu.make_async_copy(got, got, r_y).wait()
    fw = pltpu.make_async_remote_copy(
        src_ref=y_v.at[rows], dst_ref=y_v.at[rows], send_sem=s_f, recv_sem=r_f,
        device_id={'emb': e, 'model': om})
    fw.start()
    out0 = pltpu.make_async_copy(y_v.at[rows], y_h.at[rows], sem_out.at[0])
    out0.start()
    fw.wait_recv()
    orow = pl.ds(pl.multiple_of(om * bh, bh), bh)
    out1 = pltpu.make_async_copy(y_v.at[orow], y_h.at[orow], sem_out.at[1])
    out1.start()
    ex.wait_send()
    fw.wait_send()
    pltpu.make_async_copy(rest, rest, s_q).wait()
    pltpu.make_async_copy(most, most, s_o).wait()
    pltpu.make_async_copy(got, got, s_y).wait()
    out0.wait()
    out1.wait()


def solution(mesh):
    ne = mesh.shape['emb']
    nm = mesh.shape['model']
    side = round(ne ** (1 / 3))

    def local(x, Wq, Wk, Wv, Wo, Kc, Vc, lengths):
        B, D = x.shape
        DE, CQ = Wq.shape
        DH = Wk.shape[1]
        T = Kc.shape[1]
        HL = CQ // DH
        NT = CQ // L
        DC = Wo.shape[1]
        n = ne * nm
        vm = pltpu.VMEM
        dma = pltpu.SemaphoreType.DMA
        any_ = pl.BlockSpec(memory_space=pl.ANY)
        return pl.pallas_call(
            functools.partial(_kernel, side, nm),
            out_shape=(jax.ShapeDtypeStruct((B, D), BF16),
                       jax.ShapeDtypeStruct((B, DH), BF16),
                       jax.ShapeDtypeStruct((B, DH), BF16)),
            in_specs=[any_] * 7 + [pl.BlockSpec(memory_space=pltpu.SMEM)],
            out_specs=(any_, pl.BlockSpec(memory_space=vm), pl.BlockSpec(memory_space=vm)),
            scratch_shapes=[
                vm((B, D), BF16), vm((B, DE), BF16), vm((DE, CQ), BF16), vm((2, D, DH), BF16),
                vm((CQ, DC), BF16), vm((T, DH), BF16), vm((T, DH), BF16),
                vm((B * NT, L), F32), vm((n * NT, L), F32), vm((2, B, DH), F32),
                vm((nm * HL, T), F32), vm((nm, HL, DH), BF16), vm((B, HL, DH), BF16),
                vm((DH // L, B * HL, L), F32), vm((B, DC), F32), vm((B // nm, DC), F32),
                vm((B // nm, DC), BF16), vm((B, D), BF16),
                dma((8,)), dma((2,)), dma, dma, dma, dma, dma, dma, dma, dma, dma, dma,
            ],
            compiler_params=pltpu.CompilerParams(
                collective_id=0, has_side_effects=True, vmem_limit_bytes=60 * 1024 * 1024),
            name='step',
        )(x, Wq, Wk, Wv, Wo, Kc, Vc, lengths)

    in_specs = (P('rep', None), P('emb', 'model'), P(), P(), P('model', 'emb'),
                P('rep', None, None), P('rep', None, None), P('rep'))
    out_specs = (P('rep', None), P('rep', None), P('rep', None))
    return jax.shard_map(local, mesh=mesh, in_specs=in_specs, out_specs=out_specs, check_vma=False)
```

```python
import functools

import jax
import jax.numpy as jnp
from jax import lax
from jax.experimental import pallas as pl
from jax.experimental.pallas import tpu as pltpu
from jax.sharding import PartitionSpec as P

F32 = jnp.float32
BF16 = jnp.bfloat16
L = 128


def _kernel(side, nm, x_h, wq_h, wk_h, wv_h, wo_h, kc_h, vc_h, len_s,
            y_v, kn_o, vn_o,
            x_v, xl_v, wq_v, wx_v, wkv_v, wox_v, k_v, v_v,
            qp, rq, q_v, kva, s_v, of_v, os_v, og, t_v, yp, ys, ry, yb,
            sem_l, s_w, r_w, s_x, r_x, s_q, r_q, s_o, r_o, s_e, r_e, s_y, r_y, s_f, r_f):
    ne = side ** 3
    n = ne * nm
    B, D = x_v.shape
    DE = xl_v.shape[2]
    CQ = wq_v.shape[1]
    CB = CQ // side
    DH = k_v.shape[1]
    per = DH // L
    HB = CB // DH
    NB = CB // L
    RB = wox_v.shape[0]
    T = k_v.shape[0]
    DC = wo_h.shape[1]
    bh = B // nm
    scale = DH ** -0.5

    e = lax.axis_index('emb')
    m = lax.axis_index('model')
    z, y, x = e // (side * side), (e // side) % side, e % side
    me = e * nm + m

    def chip(cz, cy, cx):
        return (cz * side + cy) * side + cx

    xs = [(x + k) % side for k in range(side)]
    ms = [(m + k) % nm for k in range(nm)]
    zy = side * side

    def plane(t):
        pz = lax.rem(z + lax.div(t, side), side)
        return pz, (pz * side + lax.rem(y + lax.rem(t, side), side)) * side

    def everyone(send):
        def group(t, skip):
            pz, base = plane(t)
            for k in range(side):
                for dm in range(nm):
                    if not skip or k or dm:
                        send((t * side + k) * nm + dm, dm, pz, base + xs[k], ms[dm])

        @pl.loop(1, zy)
        def _(u):
            group(lax.rem(u * 5, zy), False)

        group(jnp.int32(0), True)

    def line(k):
        kx, ky = k * (1 - m), k * m
        pos = (x + kx) % side * (1 - m) + (y + ky) % side * m
        return chip(z, (y + ky) % side, (x + kx) % side), pos

    bar = pltpu.get_barrier_semaphore()

    everyone(lambda d, dm, pz, pe, pm: pl.semaphore_signal(
        bar, inc=1, device_id={'emb': pe, 'model': pm}))

    loads = [
        pltpu.make_async_copy(wq_h, wq_v, sem_l.at[0]),
        pltpu.make_async_copy(x_h, x_v, sem_l.at[1]),
        pltpu.make_async_copy(wk_h, wkv_v.at[0], sem_l.at[2]),
        pltpu.make_async_copy(wv_h, wkv_v.at[1], sem_l.at[3]),
        pltpu.make_async_copy(kc_h.at[me], k_v, sem_l.at[4]),
        pltpu.make_async_copy(vc_h.at[me], v_v, sem_l.at[5]),
        pltpu.make_async_copy(wo_h.at[pl.ds(pl.multiple_of(z * RB, RB), RB)], wox_v.at[:, pl.ds(0, DC)],
                              sem_l.at[6]),
    ]
    xl = []
    for k in range(side):
        src, _pos = line((side - k) % side)
        xl.append(pltpu.make_async_copy(
            x_h.at[:, pl.ds(pl.multiple_of(src * DE, DE), DE)], xl_v.at[k], sem_l.at[7 + k]))
    loads[0].start()
    for c in xl:
        c.start()
    for c in loads[1:]:
        c.start()
    loads[0].wait()

    pl.semaphore_wait(bar, n - 1)

    wsend = []
    for k in range(1, side):
        pe, pos = line(k)
        wsend.append(pltpu.make_async_remote_copy(
            src_ref=wq_v.at[:, pl.ds(pl.multiple_of(pos * CB, CB), CB)], dst_ref=wx_v.at[k],
            send_sem=s_w.at[k], recv_sem=r_w.at[k], device_id={'emb': pe, 'model': m}))
    for c in wsend:
        c.start()
    xsend = []
    for k in range(1, side):
        pz = (z + k) % side
        xsend.append(pltpu.make_async_remote_copy(
            src_ref=wo_h.at[pl.ds(pl.multiple_of(pz * RB, RB), RB)], dst_ref=wox_v.at[:, pl.ds(k * DC, DC)],
            send_sem=s_x.at[k], recv_sem=r_x.at[k], device_id={'emb': chip(pz, y, x), 'model': m}))
    for c in xsend:
        c.start()

    loads[1].wait()
    loads[2].wait()
    loads[3].wait()
    KB = min(1024, D)
    kva[...] = jnp.zeros_like(kva)

    @pl.loop(0, D // KB)
    def _(kk):
        o = pl.multiple_of(kk * KB, KB)
        xs = x_v[:, pl.ds(o, KB)]
        kva[0] += jnp.dot(xs, wkv_v[0, pl.ds(o, KB), :], preferred_element_type=F32)
        kva[1] += jnp.dot(xs, wkv_v[1, pl.ds(o, KB), :], preferred_element_type=F32)

    kn_o[...] = kva[0].astype(BF16)
    vn_o[...] = kva[1].astype(BF16)

    for c in xl:
        c.wait()
    _e, pos0 = line(0)
    for c in wsend:
        c.wait_recv()
    GN = min(4, NB)
    for j0 in range(0, NB, GN):
        t = jnp.dot(xl_v[0], wq_v[:, pl.ds(pl.multiple_of(pos0 * CB + j0 * L, L), GN * L)],
                    preferred_element_type=F32)
        for k in range(1, side):
            t = t + jnp.dot(xl_v[k], wx_v[k, :, j0 * L:(j0 + GN) * L], preferred_element_type=F32)
        for u in range(GN):
            j = j0 + u
            row = (j % per) * HB + j // per
            qp[pl.ds(row, B, stride=NB), :] = t[:, u * L:(u + 1) * L]

    def send_q(d, dm, pz, pe, pm):
        b = pe * nm + pm
        pltpu.make_async_remote_copy(
            src_ref=qp.at[pl.ds(pl.multiple_of(b * NB, NB), NB)],
            dst_ref=rq.at[pl.ds(pl.multiple_of(d * NB, NB), NB)],
            send_sem=s_q, recv_sem=r_q, device_id={'emb': pe, 'model': pm},
        ).start()

    everyone(send_q)

    rq[0:NB, :] = qp[pl.ds(pl.multiple_of(me * NB, NB), NB), :]
    loads[4].wait()
    loads[5].wait()
    rest = rq.at[pl.ds(NB, (n - 1) * NB)]
    pltpu.make_async_copy(rest, rest, r_q).wait()

    for s in range(nm):
        dm = (m + nm - s) % nm
        for j in range(side):
            acc = None
            for a in range(side):
                for b in range(side):
                    c = (a * side + b) * side + j if s == 0 else (a * side + j) * side + b
                    v = rq[pl.ds(pl.multiple_of((c * nm + dm) * NB, NB), NB), :]
                    acc = v if acc is None else acc + v
            r0 = (s * side + j) * HB
            for u in range(per):
                q_v[r0:r0 + HB, u * L:(u + 1) * L] = acc[u * HB:(u + 1) * HB]
    q = q_v[...].astype(BF16)

    kn = kva[0, pl.ds(me, 1), :].astype(BF16).astype(F32)
    vn = kva[1, pl.ds(me, 1), :].astype(BF16).astype(F32)
    sn = jnp.sum(q.astype(F32) * kn, axis=1, keepdims=True) * scale
    ln = len_s[me]
    TB = min(1024, T)
    mx = sn
    for t0 in range(0, T, TB):
        s = lax.dot_general(q, k_v[t0:t0 + TB, :], (((1,), (1,)), ((), ())),
                            preferred_element_type=F32) * scale
        tpos = lax.broadcasted_iota(jnp.int32, s.shape, 1) + t0
        s = jnp.where(tpos < ln, s, -jnp.inf)
        s_v[:, t0:t0 + TB] = s
        mx = jnp.maximum(mx, jnp.max(s, axis=1, keepdims=True))
    pn = jnp.exp(sn - mx)
    l = pn
    acc = pn.astype(BF16).astype(F32) * vn
    for t0 in range(0, T, TB):
        p = jnp.exp(s_v[:, t0:t0 + TB] - mx)
        l = l + jnp.sum(p, axis=1, keepdims=True)
        acc = acc + jnp.dot(p.astype(BF16), v_v[t0:t0 + TB, :], preferred_element_type=F32)
    o = acc / l
    for i in range(nm * side):
        for u in range(per):
            of_v[i * NB + u * HB:i * NB + (u + 1) * HB, :] = o[i * HB:(i + 1) * HB, u * L:(u + 1) * L]
    os_v[...] = of_v[...].reshape(nm * side, NB, L).astype(BF16)

    home = [x * (1 - pm) + y * pm + side for pm in ms]

    def send_o(d, dm, pz, pe, pm):
        pltpu.make_async_remote_copy(
            src_ref=os_v.at[pm * side + lax.rem(home[dm] - pz, side)], dst_ref=og.at[me],
            send_sem=s_o, recv_sem=r_o, device_id={'emb': pe, 'model': pm},
        ).start()

    everyone(send_o)
    og[me] = os_v[m * side + lax.rem(home[0] - z, side)]
    loads[6].wait()
    for c in xsend:
        c.wait_recv()
    most = og.at[pl.ds(0, n - 1)]
    pltpu.make_async_copy(most, most, r_o).wait()

    t_v[...] = og[...].astype(F32).reshape(B * NB, L)
    ya = None
    for h in range(HB):
        lhs = jnp.concatenate(
            [t_v[pl.ds(u * HB + h, B, stride=NB), :] for u in range(per)], axis=1).astype(BF16)
        t = jnp.dot(lhs, wox_v[h * DH:(h + 1) * DH, :], preferred_element_type=F32)
        ya = t if ya is None else ya + t
    yp[...] = ya[:, :DC]
    for k in range(side):
        ys[k] = ya[:, k * DC:(k + 1) * DC].astype(BF16)

    for k in range(side):
        for dm in range(nm):
            if k or dm:
                pe = chip((z + side - k) % side, y, x)
                pm = (m + dm) % nm
                pltpu.make_async_remote_copy(
                    src_ref=ys.at[k, pl.ds(pl.multiple_of(pm * bh, bh), bh)], dst_ref=ry.at[k * nm + dm],
                    send_sem=s_e, recv_sem=r_e, device_id={'emb': pe, 'model': pm}).start()
    parts = ry.at[pl.ds(1, side * nm - 1)]
    pltpu.make_async_copy(parts, parts, r_e).wait()
    rows = pl.ds(pl.multiple_of(m * bh, bh), bh)
    tot = yp[rows, :]
    for k in range(1, side * nm):
        tot = tot + ry[k].astype(F32)
    yb[...] = (xl_v[0, rows, :].astype(F32) + tot).astype(BF16)

    ycol = pl.ds(pl.multiple_of(e * DC, DC), DC)

    om = ms[1 % nm]
    hops = [side // 2] + [k for k in range(1, side) if k != side // 2] + [0]

    for dz in hops:
        def send_y(dy, _, dz=dz, skip=False):
            _pz, base = plane(dz * side + dy)
            for k in range(1 if skip else 0, side):
                pltpu.make_async_remote_copy(
                    src_ref=yb, dst_ref=y_v.at[rows, ycol], send_sem=s_y, recv_sem=r_y.at[dz],
                    device_id={'emb': base + xs[k], 'model': m},
                ).start()
            return 0

        lax.fori_loop(1 if dz == 0 else 0, side, send_y, 0)
        if dz == 0:
            send_y(jnp.int32(0), 0, skip=True)

    y_v[rows, ycol] = yb[...]
    fws = []
    for dz in hops:
        cnt = zy - (1 if dz == 0 else 0)
        got = y_v.at[pl.ds(0, bh), pl.ds(0, cnt * DC)]
        pltpu.make_async_copy(got, got, r_y.at[dz]).wait()
        cz = lax.rem(z + side - dz, side)
        span = y_v.at[rows, pl.ds(pl.multiple_of(cz * zy * DC, zy * DC), zy * DC)]
        fw = pltpu.make_async_remote_copy(
            src_ref=span, dst_ref=span, send_sem=s_f.at[dz], recv_sem=r_f.at[dz],
            device_id={'emb': e, 'model': om})
        fw.start()
        fws.append(fw)
    for c in wsend + xsend:
        c.wait_send()
    pltpu.make_async_copy(rest, rest, s_q).wait()
    pltpu.make_async_copy(most, most, s_o).wait()
    pltpu.make_async_copy(parts, parts, s_e).wait()
    allof = y_v.at[pl.ds(0, bh), pl.ds(0, (ne - 1) * DC)]
    pltpu.make_async_copy(allof, allof, s_y).wait()
    for fw in fws:
        fw.wait()


def _emit(*refs):
    k = (len(refs) - 1) // 2
    sem = refs[-1]
    cs = [pltpu.make_async_copy(refs[i], refs[k + i], sem.at[i]) for i in range(k)]
    for c in cs:
        c.start()
    for c in cs:
        c.wait()


def solution(mesh):
    ne = mesh.shape['emb']
    nm = mesh.shape['model']
    side = round(ne ** (1 / 3))

    def local(x, Wq, Wk, Wv, Wo, Kc, Vc, lengths):
        B, D = x.shape
        DE, CQ = Wq.shape
        DH = Wk.shape[1]
        T = Kc.shape[1]
        CB = CQ // side
        NB = CB // L
        HL = CQ // DH
        DC = Wo.shape[1]
        n = ne * nm
        bh = B // nm
        vm = pltpu.VMEM
        dma = pltpu.SemaphoreType.DMA
        any_ = pl.BlockSpec(memory_space=pltpu.HBM)
        vms = pl.BlockSpec(memory_space=vm)
        outs = ((B, D), (B, DH), (B, DH))
        res = pl.pallas_call(
            functools.partial(_kernel, side, nm),
            out_shape=tuple(vm(s, BF16) for s in outs),
            in_specs=[any_] * 7 + [pl.BlockSpec(memory_space=pltpu.SMEM)],
            out_specs=(vms, vms, vms),
            scratch_shapes=[
                vm((B, D), BF16), vm((side, B, DE), BF16), vm((DE, CQ), BF16), vm((side, DE, CB), BF16),
                vm((2, D, DH), BF16), vm((CB, side * DC), BF16), vm((T, DH), BF16), vm((T, DH), BF16),
                vm((B * NB, L), F32), vm((n * NB, L), F32), vm((nm * HL, DH), F32), vm((2, B, DH), F32),
                vm((nm * HL, T), F32), vm((nm * side * NB, L), F32), vm((nm * side, NB, L), BF16),
                vm((B, NB, L), BF16), vm((B * NB, L), F32), vm((B, DC), F32), vm((side, B, DC), BF16),
                vm((side * nm, bh, DC), BF16), vm((bh, DC), BF16),
                dma((7 + side,)), dma((side,)), dma((side,)), dma((side,)), dma((side,)),
                dma, dma, dma, dma, dma, dma, dma, dma((side,)), dma((side,)), dma((side,)),
            ],
            compiler_params=pltpu.CompilerParams(
                collective_id=0, has_side_effects=True, vmem_limit_bytes=61 * 1024 * 1024),
            name='step',
        )(x, Wq, Wk, Wv, Wo, Kc, Vc, lengths)
        return pl.pallas_call(
            _emit,
            out_shape=tuple(jax.ShapeDtypeStruct(s, BF16) for s in outs),
            in_specs=[vms] * 3,
            out_specs=(any_,) * 3,
            scratch_shapes=[dma((3,))],
            compiler_params=pltpu.CompilerParams(vmem_limit_bytes=1024 * 1024),
            name='emit',
        )(*[pltpu.with_memory_space_constraint(r, pltpu.VMEM) for r in res])

    in_specs = (P('rep', None), P('emb', 'model'), P(), P(), P('model', 'emb'),
                P('rep', None, None), P('rep', None, None), P('rep'))
    out_specs = (P('rep', None), P('rep', None), P('rep', None))
    return jax.shard_map(local, mesh=mesh, in_specs=in_specs, out_specs=out_specs, check_vma=False)
```

```python
import functools

import jax
import jax.numpy as jnp
from jax import lax
from jax.experimental import pallas as pl
from jax.experimental.pallas import tpu as pltpu
from jax.sharding import PartitionSpec as P

F32 = jnp.float32
BF16 = jnp.bfloat16
L = 128


def _kernel(side, nm, x_h, wq_h, wk_h, wv_h, wo_h, kc_h, vc_h, len_s,
            y_v, kn_o, vn_o,
            x_v, xl_v, wq_v, wx_v, wkv_v, wox_v, k_v, v_v,
            qp, rq, q_v, kva, s_v, of_v, os_v, og, t_v, yp, ys, ry, yb,
            sem_l, s_w, r_w, s_x, r_x, s_q, r_q, s_o, r_o, s_e, r_e, s_y, r_y, r_z, s_f, r_f, s_b):
    ne = side ** 3
    n = ne * nm
    B, D = x_v.shape
    DE = xl_v.shape[2]
    CQ = wq_v.shape[1]
    CB = CQ // side
    DH = k_v.shape[1]
    per = DH // L
    HB = CB // DH
    NB = CB // L
    RB = wox_v.shape[0]
    T = k_v.shape[0]
    DC = wo_h.shape[1]
    bh = B // nm
    scale = DH ** -0.5

    e = lax.axis_index('emb')
    m = lax.axis_index('model')
    z, y, x = e // (side * side), (e // side) % side, e % side
    me = e * nm + m

    def chip(cz, cy, cx):
        return (cz * side + cy) * side + cx

    xs = [(x + k) % side for k in range(side)]
    ms = [(m + k) % nm for k in range(nm)]
    zy = side * side

    def plane(t):
        pz = lax.rem(z + lax.div(t, side), side)
        return pz, (pz * side + lax.rem(y + lax.rem(t, side), side)) * side

    def everyone(send):
        def group(t, skip):
            pz, base = plane(t)
            for k in range(side):
                for dm in range(nm):
                    if not skip or k or dm:
                        send((t * side + k) * nm + dm, dm, pz, base + xs[k], ms[dm])

        @pl.loop(1, zy)
        def _(u):
            group(lax.rem(u * 5, zy), False)

        group(jnp.int32(0), True)

    def line(k):
        kx, ky = k * (1 - m), k * m
        pos = (x + kx) % side * (1 - m) + (y + ky) % side * m
        return chip(z, (y + ky) % side, (x + kx) % side), pos

    bar = pltpu.get_barrier_semaphore()

    def greet(sem, pe, pm):
        pl.semaphore_signal(sem, inc=1, device_id={'emb': pe, 'model': pm})

    ly = [chip(z, lax.rem(y + k, side), x) for k in range(1, side)]
    lz = [chip(lax.rem(z + k, side), y, x) for k in range(1, side)]
    for k in range(side):
        for dm in range(nm):
            if k or dm:
                greet(bar, chip(z, y, xs[k]), ms[dm])
    for pe in ly + lz:
        greet(bar, pe, m)

    loads = [
        pltpu.make_async_copy(wq_h, wq_v, sem_l.at[0]),
        pltpu.make_async_copy(x_h, x_v, sem_l.at[1]),
        pltpu.make_async_copy(wk_h, wkv_v.at[0], sem_l.at[2]),
        pltpu.make_async_copy(wv_h, wkv_v.at[1], sem_l.at[3]),
        pltpu.make_async_copy(kc_h.at[me], k_v, sem_l.at[4]),
        pltpu.make_async_copy(vc_h.at[me], v_v, sem_l.at[5]),
        pltpu.make_async_copy(wo_h.at[pl.ds(pl.multiple_of(z * RB, RB), RB)], wox_v.at[:, pl.ds(0, DC)],
                              sem_l.at[6]),
    ]
    xl = []
    for k in range(side):
        src, _pos = line((side - k) % side)
        xl.append(pltpu.make_async_copy(
            x_h.at[:, pl.ds(pl.multiple_of(src * DE, DE), DE)], xl_v.at[k], sem_l.at[7 + k]))
    loads[0].start()
    for c in xl:
        c.start()
    for c in loads[1:]:
        c.start()
    loads[0].wait()

    pl.semaphore_wait(bar, side * nm - 1 + 2 * (side - 1))

    wsend = []
    for k in range(1, side):
        pe, pos = line(k)
        wsend.append(pltpu.make_async_remote_copy(
            src_ref=wq_v.at[:, pl.ds(pl.multiple_of(pos * CB, CB), CB)], dst_ref=wx_v.at[k],
            send_sem=s_w.at[k], recv_sem=r_w.at[k], device_id={'emb': pe, 'model': m}))
    for c in wsend:
        c.start()
    xsend = []
    for k in range(1, side):
        pz = (z + k) % side
        xsend.append(pltpu.make_async_remote_copy(
            src_ref=wo_h.at[pl.ds(pl.multiple_of(pz * RB, RB), RB)], dst_ref=wox_v.at[:, pl.ds(k * DC, DC)],
            send_sem=s_x.at[k], recv_sem=r_x.at[k], device_id={'emb': chip(pz, y, x), 'model': m}))
    for c in xsend:
        c.start()
    for pe in ly:
        greet(s_b.at[0], pe, m)
    pl.semaphore_wait(s_b.at[0], side - 1)
    for pe in lz:
        greet(s_b.at[1], pe, m)

    loads[1].wait()
    loads[2].wait()
    loads[3].wait()
    KB = min(1024, D)
    kva[...] = jnp.zeros_like(kva)

    @pl.loop(0, D // KB)
    def _(kk):
        o = pl.multiple_of(kk * KB, KB)
        xs = x_v[:, pl.ds(o, KB)]
        kva[0] += jnp.dot(xs, wkv_v[0, pl.ds(o, KB), :], preferred_element_type=F32)
        kva[1] += jnp.dot(xs, wkv_v[1, pl.ds(o, KB), :], preferred_element_type=F32)

    kn_o[...] = kva[0].astype(BF16)
    vn_o[...] = kva[1].astype(BF16)

    pl.semaphore_wait(s_b.at[1], side - 1)
    for c in xl:
        c.wait()
    _e, pos0 = line(0)
    for c in wsend:
        c.wait_recv()
    GN = min(4, NB)
    for j0 in range(0, NB, GN):
        t = jnp.dot(xl_v[0], wq_v[:, pl.ds(pl.multiple_of(pos0 * CB + j0 * L, L), GN * L)],
                    preferred_element_type=F32)
        for k in range(1, side):
            t = t + jnp.dot(xl_v[k], wx_v[k, :, j0 * L:(j0 + GN) * L], preferred_element_type=F32)
        for u in range(GN):
            j = j0 + u
            row = (j % per) * HB + j // per
            qp[pl.ds(row, B, stride=NB), :] = t[:, u * L:(u + 1) * L]

    def send_q(d, dm, pz, pe, pm):
        b = pe * nm + pm
        pltpu.make_async_remote_copy(
            src_ref=qp.at[pl.ds(pl.multiple_of(b * NB, NB), NB)],
            dst_ref=rq.at[pl.ds(pl.multiple_of(d * NB, NB), NB)],
            send_sem=s_q, recv_sem=r_q, device_id={'emb': pe, 'model': pm},
        ).start()

    everyone(send_q)

    rq[0:NB, :] = qp[pl.ds(pl.multiple_of(me * NB, NB), NB), :]
    loads[4].wait()
    loads[5].wait()
    rest = rq.at[pl.ds(NB, (n - 1) * NB)]
    pltpu.make_async_copy(rest, rest, r_q).wait()

    for s in range(nm):
        dm = (m + nm - s) % nm
        for j in range(side):
            acc = None
            for a in range(side):
                for b in range(side):
                    c = (a * side + b) * side + j if s == 0 else (a * side + j) * side + b
                    v = rq[pl.ds(pl.multiple_of((c * nm + dm) * NB, NB), NB), :]
                    acc = v if acc is None else acc + v
            r0 = (s * side + j) * HB
            for u in range(per):
                q_v[r0:r0 + HB, u * L:(u + 1) * L] = acc[u * HB:(u + 1) * HB]
    q = q_v[...].astype(BF16)

    kn = kva[0, pl.ds(me, 1), :].astype(BF16).astype(F32)
    vn = kva[1, pl.ds(me, 1), :].astype(BF16).astype(F32)
    sn = jnp.sum(q.astype(F32) * kn, axis=1, keepdims=True) * scale
    ln = len_s[me]
    TB = min(1024, T)
    mx = sn
    for t0 in range(0, T, TB):
        s = lax.dot_general(q, k_v[t0:t0 + TB, :], (((1,), (1,)), ((), ())),
                            preferred_element_type=F32) * scale
        tpos = lax.broadcasted_iota(jnp.int32, s.shape, 1) + t0
        s = jnp.where(tpos < ln, s, -jnp.inf)
        s_v[:, t0:t0 + TB] = s
        mx = jnp.maximum(mx, jnp.max(s, axis=1, keepdims=True))
    pn = jnp.exp(sn - mx)
    l = pn
    acc = pn.astype(BF16).astype(F32) * vn
    for t0 in range(0, T, TB):
        p = jnp.exp(s_v[:, t0:t0 + TB] - mx)
        l = l + jnp.sum(p, axis=1, keepdims=True)
        acc = acc + jnp.dot(p.astype(BF16), v_v[t0:t0 + TB, :], preferred_element_type=F32)
    o = acc / l
    for i in range(nm * side):
        for u in range(per):
            of_v[i * NB + u * HB:i * NB + (u + 1) * HB, :] = o[i * HB:(i + 1) * HB, u * L:(u + 1) * L]
    os_v[...] = of_v[...].reshape(nm * side, NB, L).astype(BF16)

    home = [x * (1 - pm) + y * pm + side for pm in ms]

    def send_o(d, dm, pz, pe, pm):
        pltpu.make_async_remote_copy(
            src_ref=os_v.at[pm * side + lax.rem(home[dm] - pz, side)], dst_ref=og.at[me],
            send_sem=s_o, recv_sem=r_o, device_id={'emb': pe, 'model': pm},
        ).start()

    everyone(send_o)
    og[me] = os_v[m * side + lax.rem(home[0] - z, side)]
    loads[6].wait()
    for c in xsend:
        c.wait_recv()
    most = og.at[pl.ds(0, n - 1)]
    pltpu.make_async_copy(most, most, r_o).wait()

    t_v[...] = og[...].astype(F32).reshape(B * NB, L)
    ya = None
    for h in range(HB):
        lhs = jnp.concatenate(
            [t_v[pl.ds(u * HB + h, B, stride=NB), :] for u in range(per)], axis=1).astype(BF16)
        t = jnp.dot(lhs, wox_v[h * DH:(h + 1) * DH, :], preferred_element_type=F32)
        ya = t if ya is None else ya + t
    yp[...] = ya[:, :DC]
    for k in range(side):
        ys[k] = ya[:, k * DC:(k + 1) * DC].astype(BF16)

    for k in range(side):
        for dm in range(nm):
            if k or dm:
                pe = chip((z + side - k) % side, y, x)
                pm = (m + dm) % nm
                pltpu.make_async_remote_copy(
                    src_ref=ys.at[k, pl.ds(pl.multiple_of(pm * bh, bh), bh)], dst_ref=ry.at[k * nm + dm],
                    send_sem=s_e, recv_sem=r_e, device_id={'emb': pe, 'model': pm}).start()
    parts = ry.at[pl.ds(1, side * nm - 1)]
    pltpu.make_async_copy(parts, parts, r_e).wait()
    rows = pl.ds(pl.multiple_of(m * bh, bh), bh)
    tot = yp[rows, :]
    for k in range(1, side * nm):
        tot = tot + ry[k].astype(F32)
    yb[...] = (xl_v[0, rows, :].astype(F32) + tot).astype(BF16)

    ycol = pl.ds(pl.multiple_of(e * DC, DC), DC)

    om = ms[1 % nm]
    rb = min(8, bh // 8)
    cuts = [0, (bh // rb + 2) // 3 * rb]
    cuts += [min(bh, cuts[1] * 2), bh]
    far = [side // 2] + [k for k in range(1, side) if k != side // 2]
    here = (z, y, x)

    def move(offs):
        c = [h if o is None else lax.rem(h + side + o, side) for h, o in zip(here, offs)]
        return chip(*c)

    def offsets(axis, da, db, dl):
        o = [da, db]
        o.insert(axis, dl)
        return o

    def piece(c, src):
        return y_v.at[pl.ds(pl.multiple_of(m * bh + cuts[c], rb), cuts[c + 1] - cuts[c]),
                      pl.ds(pl.multiple_of(src * DC, DC), DC)]

    def mine(c):
        return yb.at[pl.ds(cuts[c], cuts[c + 1] - cuts[c])]

    def push(src_ref, dst_ref, sem, pe):
        pltpu.make_async_remote_copy(
            src_ref=src_ref, dst_ref=dst_ref, send_sem=s_y, recv_sem=sem,
            device_id={'emb': pe, 'model': m}).start()

    for da in far + [0]:
        def spread(db, _, da=da):
            for c in range(3):
                push(mine(c), piece(c, e), r_y.at[c, da], move(offsets(c, da, db, None)))
            return 0
        lax.fori_loop(1 if da == 0 else 0, side, spread, 0)
    for c in range(3):
        for dl in far:
            push(mine(c), piece(c, e), r_z.at[c], move(offsets(c, None, None, dl)))
    y_v[rows, ycol] = yb[...]

    for da in [0] + far[::-1]:
        for c in range(3):
            got = y_v.at[pl.ds(0, cuts[c + 1] - cuts[c]), pl.ds(0, (side - (da == 0)) * DC)]
            pltpu.make_async_copy(got, got, r_y.at[c, da]).wait()

            def relay(db, _, da=da, c=c):
                ref = piece(c, move(offsets(c, -da, -db, None)))
                for dl in far:
                    push(ref, ref, r_z.at[c], move(offsets(c, None, None, dl)))
                return 0
            lax.fori_loop(1 if da == 0 else 0, side, relay, 0)

    fws = []
    for c in range(3):
        got = y_v.at[pl.ds(0, cuts[c + 1] - cuts[c]), pl.ds(0, (side - 1) * zy * DC)]
        pltpu.make_async_copy(got, got, r_z.at[c]).wait()
        span = y_v.at[pl.ds(pl.multiple_of(m * bh + cuts[c], rb), cuts[c + 1] - cuts[c])]
        fw = pltpu.make_async_remote_copy(
            src_ref=span, dst_ref=span, send_sem=s_f.at[c], recv_sem=r_f.at[c],
            device_id={'emb': e, 'model': om})
        fw.start()
        fws.append(fw)
    for c in wsend + xsend:
        c.wait_send()
    pltpu.make_async_copy(rest, rest, s_q).wait()
    pltpu.make_async_copy(most, most, s_o).wait()
    pltpu.make_async_copy(parts, parts, s_e).wait()
    allof = y_v.at[pl.ds(0, bh), pl.ds(0, (ne - 1) * DC)]
    pltpu.make_async_copy(allof, allof, s_y).wait()
    for fw in fws:
        fw.wait()


def _emit(*refs):
    k = (len(refs) - 1) // 2
    sem = refs[-1]
    cs = [pltpu.make_async_copy(refs[i], refs[k + i], sem.at[i]) for i in range(k)]
    for c in cs:
        c.start()
    for c in cs:
        c.wait()


def solution(mesh):
    ne = mesh.shape['emb']
    nm = mesh.shape['model']
    side = round(ne ** (1 / 3))

    def local(x, Wq, Wk, Wv, Wo, Kc, Vc, lengths):
        B, D = x.shape
        DE, CQ = Wq.shape
        DH = Wk.shape[1]
        T = Kc.shape[1]
        CB = CQ // side
        NB = CB // L
        HL = CQ // DH
        DC = Wo.shape[1]
        n = ne * nm
        bh = B // nm
        vm = pltpu.VMEM
        dma = pltpu.SemaphoreType.DMA
        any_ = pl.BlockSpec(memory_space=pltpu.HBM)
        vms = pl.BlockSpec(memory_space=vm)
        outs = ((B, D), (B, DH), (B, DH))
        res = pl.pallas_call(
            functools.partial(_kernel, side, nm),
            out_shape=tuple(vm(s, BF16) for s in outs),
            in_specs=[any_] * 7 + [pl.BlockSpec(memory_space=pltpu.SMEM)],
            out_specs=(vms, vms, vms),
            scratch_shapes=[
                vm((B, D), BF16), vm((side, B, DE), BF16), vm((DE, CQ), BF16), vm((side, DE, CB), BF16),
                vm((2, D, DH), BF16), vm((CB, side * DC), BF16), vm((T, DH), BF16), vm((T, DH), BF16),
                vm((B * NB, L), F32), vm((n * NB, L), F32), vm((nm * HL, DH), F32), vm((2, B, DH), F32),
                vm((nm * HL, T), F32), vm((nm * side * NB, L), F32), vm((nm * side, NB, L), BF16),
                vm((B, NB, L), BF16), vm((B * NB, L), F32), vm((B, DC), F32), vm((side, B, DC), BF16),
                vm((side * nm, bh, DC), BF16), vm((bh, DC), BF16),
                dma((7 + side,)), dma((side,)), dma((side,)), dma((side,)), dma((side,)),
                dma, dma, dma, dma, dma, dma, dma, dma((3, side)), dma((3,)), dma((3,)), dma((3,)),
                pltpu.SemaphoreType.REGULAR((2,)),
            ],
            compiler_params=pltpu.CompilerParams(
                collective_id=0, has_side_effects=True, vmem_limit_bytes=61 * 1024 * 1024),
            name='step',
        )(x, Wq, Wk, Wv, Wo, Kc, Vc, lengths)
        return pl.pallas_call(
            _emit,
            out_shape=tuple(jax.ShapeDtypeStruct(s, BF16) for s in outs),
            in_specs=[vms] * 3,
            out_specs=(any_,) * 3,
            scratch_shapes=[dma((3,))],
            compiler_params=pltpu.CompilerParams(vmem_limit_bytes=1024 * 1024),
            name='emit',
        )(*[pltpu.with_memory_space_constraint(r, pltpu.VMEM) for r in res])

    in_specs = (P('rep', None), P('emb', 'model'), P(), P(), P('model', 'emb'),
                P('rep', None, None), P('rep', None, None), P('rep'))
    out_specs = (P('rep', None), P('rep', None), P('rep', None))
    return jax.shard_map(local, mesh=mesh, in_specs=in_specs, out_specs=out_specs, check_vma=False)
```

```python
import functools

import jax
import jax.numpy as jnp
from jax import lax
from jax.experimental import pallas as pl
from jax.experimental.pallas import tpu as pltpu
from jax.sharding import PartitionSpec as P

F32 = jnp.float32
BF16 = jnp.bfloat16
L = 128


def _kernel(side, nm, x_h, wq_h, wk_h, wv_h, wo_h, kc_h, vc_h, len_s,
            y_v, kn_o, vn_o,
            x_v, xl_v, wq_v, wx_v, wkv_v, wox_v, k_v, v_v,
            qp, rq, q_v, kva, s_v, of_v, os_v, og, t_v, yp, ys, ry, yb,
            sem_l, s_w, r_w, s_x, r_x, s_q, r_q, s_o, r_o, s_e, r_e, s_y, r_y, r_z, s_f, r_f, s_b):
    ne = side ** 3
    n = ne * nm
    B, D = x_v.shape
    DE = xl_v.shape[2]
    CQ = wq_v.shape[1]
    CB = CQ // side
    DH = k_v.shape[1]
    per = DH // L
    HB = CB // DH
    NB = CB // L
    NC = qp.shape[0]
    CC = CB // NC
    HC = HB // NC
    RC = NB // NC
    RB = wox_v.shape[0]
    T = k_v.shape[0]
    DC = wo_h.shape[1]
    bh = B // nm
    scale = DH ** -0.5

    e = lax.axis_index('emb')
    m = lax.axis_index('model')
    z, y, x = e // (side * side), (e // side) % side, e % side
    me = e * nm + m

    def chip(cz, cy, cx):
        return (cz * side + cy) * side + cx

    xs = [(x + k) % side for k in range(side)]
    ms = [(m + k) % nm for k in range(nm)]
    zy = side * side
    far = [side // 2] + [k for k in range(1, side) if k != side // 2]

    def plane(t):
        pz = lax.rem(z + lax.div(t, side), side)
        return pz, (pz * side + lax.rem(y + lax.rem(t, side), side)) * side

    def everyone(send):
        def group(t, skip):
            pz, base = plane(t)
            for k in range(side):
                for dm in range(nm):
                    if not skip or k or dm:
                        send((t * side + k) * nm + dm, dm, pz, base + xs[k], ms[dm])

        @pl.loop(1, zy)
        def _(u):
            group(lax.rem(u * 5, zy), False)

        group(jnp.int32(0), True)

    def line(k):
        kx, ky = k * (1 - m), k * m
        pos = (x + kx) % side * (1 - m) + (y + ky) % side * m
        return chip(z, (y + ky) % side, (x + kx) % side), pos

    bar = pltpu.get_barrier_semaphore()

    def greet(sem, pe, pm):
        pl.semaphore_signal(sem, inc=1, device_id={'emb': pe, 'model': pm})

    ly = [chip(z, lax.rem(y + k, side), x) for k in range(1, side)]
    lz = [chip(lax.rem(z + k, side), y, x) for k in range(1, side)]
    for k in range(side):
        for dm in range(nm):
            if k or dm:
                greet(bar, chip(z, y, xs[k]), ms[dm])
    for pe in ly + lz:
        greet(bar, pe, m)

    loads = [
        pltpu.make_async_copy(wq_h, wq_v, sem_l.at[0]),
        pltpu.make_async_copy(x_h, x_v, sem_l.at[1]),
        pltpu.make_async_copy(wk_h, wkv_v.at[0], sem_l.at[2]),
        pltpu.make_async_copy(wv_h, wkv_v.at[1], sem_l.at[3]),
        pltpu.make_async_copy(kc_h.at[me], k_v, sem_l.at[4]),
        pltpu.make_async_copy(vc_h.at[me], v_v, sem_l.at[5]),
        pltpu.make_async_copy(wo_h.at[pl.ds(pl.multiple_of(z * RB, RB), RB)], wox_v.at[:, pl.ds(0, DC)],
                              sem_l.at[6]),
    ]
    xl = []
    for k in range(side):
        src, _pos = line((side - k) % side)
        xl.append(pltpu.make_async_copy(
            x_h.at[:, pl.ds(pl.multiple_of(src * DE, DE), DE)], xl_v.at[k], sem_l.at[7 + k]))
    loads[0].start()
    for c in xl:
        c.start()
    for c in loads[1:]:
        c.start()
    loads[0].wait()

    pl.semaphore_wait(bar, side * nm - 1 + 2 * (side - 1))

    wsend = []
    for h in range(NC):
        for k in far:
            pe, pos = line(k)
            wsend.append(pltpu.make_async_remote_copy(
                src_ref=wq_v.at[:, pl.ds(pl.multiple_of(pos * CB + h * CC, CC), CC)],
                dst_ref=wx_v.at[k, :, pl.ds(h * CC, CC)],
                send_sem=s_w.at[h, k], recv_sem=r_w.at[h, k], device_id={'emb': pe, 'model': m}))
    for c in wsend:
        c.start()
    xsend = []
    for k in range(1, side):
        pz = (z + k) % side
        xsend.append(pltpu.make_async_remote_copy(
            src_ref=wo_h.at[pl.ds(pl.multiple_of(pz * RB, RB), RB)], dst_ref=wox_v.at[:, pl.ds(k * DC, DC)],
            send_sem=s_x.at[k], recv_sem=r_x.at[k], device_id={'emb': chip(pz, y, x), 'model': m}))
    for c in xsend:
        c.start()
    for pe in ly:
        greet(s_b.at[0], pe, m)
    pl.semaphore_wait(s_b.at[0], side - 1)
    for pe in lz:
        greet(s_b.at[1], pe, m)

    loads[1].wait()
    loads[2].wait()
    loads[3].wait()
    KB = min(1024, D)
    kva[...] = jnp.zeros_like(kva)

    @pl.loop(0, D // KB)
    def _(kk):
        o = pl.multiple_of(kk * KB, KB)
        xs = x_v[:, pl.ds(o, KB)]
        kva[0] += jnp.dot(xs, wkv_v[0, pl.ds(o, KB), :], preferred_element_type=F32)
        kva[1] += jnp.dot(xs, wkv_v[1, pl.ds(o, KB), :], preferred_element_type=F32)

    kn_o[...] = kva[0].astype(BF16)
    vn_o[...] = kva[1].astype(BF16)

    pl.semaphore_wait(s_b.at[1], side - 1)
    for c in xl:
        c.wait()
    _e, pos0 = line(0)
    for h in range(NC):
        for c in wsend[h * (side - 1):(h + 1) * (side - 1)]:
            c.wait_recv()
        t = jnp.dot(xl_v[0], wq_v[:, pl.ds(pl.multiple_of(pos0 * CB + h * CC, CC), CC)],
                    preferred_element_type=F32)
        for k in range(1, side):
            t = t + jnp.dot(xl_v[k], wx_v[k, :, h * CC:(h + 1) * CC], preferred_element_type=F32)
        for j in range(RC):
            qp[h, :, (j % per) * HC + j // per, :] = t[:, j * L:(j + 1) * L]

        def send_q(d, dm, pz, pe, pm, h=h):
            pltpu.make_async_remote_copy(
                src_ref=qp.at[h, pe * nm + pm], dst_ref=rq.at[h, d],
                send_sem=s_q, recv_sem=r_q.at[h], device_id={'emb': pe, 'model': pm},
            ).start()

        everyone(send_q)
        rq[h, 0] = qp[h, me]

    loads[4].wait()
    loads[5].wait()
    for h in range(NC):
        rest = rq.at[h, pl.ds(1, n - 1)]
        pltpu.make_async_copy(rest, rest, r_q.at[h]).wait()

    for s in range(nm):
        dm = (m + nm - s) % nm
        for j in range(side):
            for h in range(NC):
                acc = None
                for a in range(side):
                    for b in range(side):
                        c = (a * side + b) * side + j if s == 0 else (a * side + j) * side + b
                        v = rq[h, c * nm + dm]
                        acc = v if acc is None else acc + v
                r0 = (s * side + j) * HB + h * HC
                for u in range(per):
                    q_v[r0:r0 + HC, u * L:(u + 1) * L] = acc[u * HC:(u + 1) * HC]
    q = q_v[...].astype(BF16)

    kn = kva[0, pl.ds(me, 1), :].astype(BF16).astype(F32)
    vn = kva[1, pl.ds(me, 1), :].astype(BF16).astype(F32)
    sn = jnp.sum(q.astype(F32) * kn, axis=1, keepdims=True) * scale
    ln = len_s[me]
    TB = min(1024, T)
    mx = sn
    for t0 in range(0, T, TB):
        s = lax.dot_general(q, k_v[t0:t0 + TB, :], (((1,), (1,)), ((), ())),
                            preferred_element_type=F32) * scale
        tpos = lax.broadcasted_iota(jnp.int32, s.shape, 1) + t0
        s = jnp.where(tpos < ln, s, -jnp.inf)
        s_v[:, t0:t0 + TB] = s
        mx = jnp.maximum(mx, jnp.max(s, axis=1, keepdims=True))
    pn = jnp.exp(sn - mx)
    l = pn
    acc = pn.astype(BF16).astype(F32) * vn
    for t0 in range(0, T, TB):
        p = jnp.exp(s_v[:, t0:t0 + TB] - mx)
        l = l + jnp.sum(p, axis=1, keepdims=True)
        acc = acc + jnp.dot(p.astype(BF16), v_v[t0:t0 + TB, :], preferred_element_type=F32)
    o = acc / l
    for i in range(nm * side):
        for u in range(per):
            of_v[i * NB + u * HB:i * NB + (u + 1) * HB, :] = o[i * HB:(i + 1) * HB, u * L:(u + 1) * L]
    os_v[...] = of_v[...].reshape(nm * side, NB, L).astype(BF16)

    home = [x * (1 - pm) + y * pm + side for pm in ms]

    def send_o(d, dm, pz, pe, pm):
        pltpu.make_async_remote_copy(
            src_ref=os_v.at[pm * side + lax.rem(home[dm] - pz, side)], dst_ref=og.at[me],
            send_sem=s_o, recv_sem=r_o, device_id={'emb': pe, 'model': pm},
        ).start()

    everyone(send_o)
    og[me] = os_v[m * side + lax.rem(home[0] - z, side)]
    loads[6].wait()
    for c in xsend:
        c.wait_recv()
    most = og.at[pl.ds(0, n - 1)]
    pltpu.make_async_copy(most, most, r_o).wait()

    t_v[...] = og[...].astype(F32).reshape(B * NB, L)
    ya = None
    for h in range(HB):
        lhs = jnp.concatenate(
            [t_v[pl.ds(u * HB + h, B, stride=NB), :] for u in range(per)], axis=1).astype(BF16)
        t = jnp.dot(lhs, wox_v[h * DH:(h + 1) * DH, :], preferred_element_type=F32)
        ya = t if ya is None else ya + t
    yp[...] = ya[:, :DC]
    for k in range(side):
        ys[k] = ya[:, k * DC:(k + 1) * DC].astype(BF16)

    for k in far + [0]:
        for dm in range(nm):
            if k or dm:
                pe = chip((z + side - k) % side, y, x)
                pm = (m + dm) % nm
                pltpu.make_async_remote_copy(
                    src_ref=ys.at[k, pl.ds(pl.multiple_of(pm * bh, bh), bh)], dst_ref=ry.at[k * nm + dm],
                    send_sem=s_e, recv_sem=r_e, device_id={'emb': pe, 'model': pm}).start()
    parts = ry.at[pl.ds(1, side * nm - 1)]
    pltpu.make_async_copy(parts, parts, r_e).wait()
    rows = pl.ds(pl.multiple_of(m * bh, bh), bh)
    tot = yp[rows, :]
    for k in range(1, side * nm):
        tot = tot + ry[k].astype(F32)
    yb[...] = (xl_v[0, rows, :].astype(F32) + tot).astype(BF16)

    ycol = pl.ds(pl.multiple_of(e * DC, DC), DC)

    om = ms[1 % nm]
    rb = min(8, bh // 8)
    cuts = [0, (bh // rb + 2) // 3 * rb]
    cuts += [min(bh, cuts[1] * 2), bh]
    here = (z, y, x)

    def move(offs):
        c = [h if o is None else lax.rem(h + side + o, side) for h, o in zip(here, offs)]
        return chip(*c)

    def offsets(axis, da, db, dl):
        o = [da, db]
        o.insert(axis, dl)
        return o

    def piece(c, src):
        return y_v.at[pl.ds(pl.multiple_of(m * bh + cuts[c], rb), cuts[c + 1] - cuts[c]),
                      pl.ds(pl.multiple_of(src * DC, DC), DC)]

    def mine(c):
        return yb.at[pl.ds(cuts[c], cuts[c + 1] - cuts[c])]

    def push(src_ref, dst_ref, sem, pe):
        pltpu.make_async_remote_copy(
            src_ref=src_ref, dst_ref=dst_ref, send_sem=s_y, recv_sem=sem,
            device_id={'emb': pe, 'model': m}).start()

    for da in far + [0]:
        def spread(db, _, da=da):
            for c in range(3):
                push(mine(c), piece(c, e), r_y.at[c, da], move(offsets(c, da, db, None)))
            return 0
        lax.fori_loop(1 if da == 0 else 0, side, spread, 0)
    for c in range(3):
        for dl in far:
            push(mine(c), piece(c, e), r_z.at[c, dl], move(offsets(c, None, None, dl)))
    y_v[rows, ycol] = yb[...]

    for da in [0] + far[::-1]:
        for c in range(3):
            got = y_v.at[pl.ds(0, cuts[c + 1] - cuts[c]), pl.ds(0, (side - (da == 0)) * DC)]
            pltpu.make_async_copy(got, got, r_y.at[c, da]).wait()

            def relay(db, _, da=da, c=c):
                ref = piece(c, move(offsets(c, -da, -db, None)))
                for dl in far:
                    push(ref, ref, r_z.at[c, dl], move(offsets(c, None, None, dl)))
                return 0
            lax.fori_loop(1 if da == 0 else 0, side, relay, 0)

    def cross(c, dl):
        at = lax.rem(here[c] + side - dl, side)
        width = side ** (2 - c) * DC

        def one(g, _):
            ref = y_v.at[pl.ds(pl.multiple_of(m * bh + cuts[c], rb), cuts[c + 1] - cuts[c]),
                         pl.ds(pl.multiple_of((g * side + at) * width, width), width)]
            pltpu.make_async_remote_copy(
                src_ref=ref, dst_ref=ref, send_sem=s_f, recv_sem=r_f,
                device_id={'emb': e, 'model': om}).start()
            return 0

        lax.fori_loop(0, side ** c, one, 0)

    for c in range(3):
        cross(c, 0)
    for dl in far[::-1]:
        for c in range(3):
            got = y_v.at[pl.ds(0, cuts[c + 1] - cuts[c]), pl.ds(0, zy * DC)]
            pltpu.make_async_copy(got, got, r_z.at[c, dl]).wait()
            cross(c, dl)
    for c in wsend + xsend:
        c.wait_send()
    allq = rq.at[:, pl.ds(1, n - 1)]
    pltpu.make_async_copy(allq, allq, s_q).wait()
    pltpu.make_async_copy(most, most, s_o).wait()
    pltpu.make_async_copy(parts, parts, s_e).wait()
    allof = y_v.at[pl.ds(0, bh), pl.ds(0, (ne - 1) * DC)]
    pltpu.make_async_copy(allof, allof, s_y).wait()
    half = y_v.at[pl.ds(0, bh)]
    pltpu.make_async_copy(half, half, s_f).wait()
    pltpu.make_async_copy(half, half, r_f).wait()


def _emit(*refs):
    k = (len(refs) - 1) // 2
    sem = refs[-1]
    cs = []
    for i in range(k):
        r = refs[i].shape[0]
        q = r // 8 if i == 0 else r
        for p in range(r // q):
            rows = pl.ds(p * q, q)
            cs.append(pltpu.make_async_copy(refs[i].at[rows], refs[k + i].at[rows], sem.at[len(cs)]))
    for c in cs:
        c.start()
    for c in cs:
        c.wait()


def solution(mesh):
    ne = mesh.shape['emb']
    nm = mesh.shape['model']
    side = round(ne ** (1 / 3))

    def local(x, Wq, Wk, Wv, Wo, Kc, Vc, lengths):
        B, D = x.shape
        DE, CQ = Wq.shape
        DH = Wk.shape[1]
        T = Kc.shape[1]
        CB = CQ // side
        NB = CB // L
        NC = 1
        HL = CQ // DH
        DC = Wo.shape[1]
        n = ne * nm
        bh = B // nm
        vm = pltpu.VMEM
        dma = pltpu.SemaphoreType.DMA
        any_ = pl.BlockSpec(memory_space=pltpu.HBM)
        vms = pl.BlockSpec(memory_space=vm)
        outs = ((B, D), (B, DH), (B, DH))
        res = pl.pallas_call(
            functools.partial(_kernel, side, nm),
            out_shape=tuple(vm(s, BF16) for s in outs),
            in_specs=[any_] * 7 + [pl.BlockSpec(memory_space=pltpu.SMEM)],
            out_specs=(vms, vms, vms),
            scratch_shapes=[
                vm((B, D), BF16), vm((side, B, DE), BF16), vm((DE, CQ), BF16), vm((side, DE, CB), BF16),
                vm((2, D, DH), BF16), vm((CB, side * DC), BF16), vm((T, DH), BF16), vm((T, DH), BF16),
                vm((NC, B, NB // NC, L), F32), vm((NC, n, NB // NC, L), F32), vm((nm * HL, DH), F32), vm((2, B, DH), F32),
                vm((nm * HL, T), F32), vm((nm * side * NB, L), F32), vm((nm * side, NB, L), BF16),
                vm((B, NB, L), BF16), vm((B * NB, L), F32), vm((B, DC), F32), vm((side, B, DC), BF16),
                vm((side * nm, bh, DC), BF16), vm((bh, DC), BF16),
                dma((7 + side,)), dma((NC, side)), dma((NC, side)), dma((side,)), dma((side,)),
                dma, dma((NC,)), dma, dma, dma, dma, dma, dma((3, side)), dma((3, side)), dma, dma,
                pltpu.SemaphoreType.REGULAR((2,)),
            ],
            compiler_params=pltpu.CompilerParams(
                collective_id=0, has_side_effects=True, vmem_limit_bytes=61 * 1024 * 1024),
            name='step',
        )(x, Wq, Wk, Wv, Wo, Kc, Vc, lengths)
        return pl.pallas_call(
            _emit,
            out_shape=tuple(jax.ShapeDtypeStruct(s, BF16) for s in outs),
            in_specs=[vms] * 3,
            out_specs=(any_,) * 3,
            scratch_shapes=[dma((10,))],
            compiler_params=pltpu.CompilerParams(vmem_limit_bytes=1024 * 1024),
            name='emit',
        )(*[pltpu.with_memory_space_constraint(r, pltpu.VMEM) for r in res])

    in_specs = (P('rep', None), P('emb', 'model'), P(), P(), P('model', 'emb'),
                P('rep', None, None), P('rep', None, None), P('rep'))
    out_specs = (P('rep', None), P('rep', None), P('rep', None))
    return jax.shard_map(local, mesh=mesh, in_specs=in_specs, out_specs=out_specs, check_vma=False)
```
